32 devices in a mesh: space: 8 (over z, y), member: 4 (over x, core).
Axes of the slice: x: 2, y: 2, z: 4, core: 2. Of those that a mesh axis runs over, the one named last changes fastest.
Arguments:
- increment: bfloat16 [768, 64, 128], P('space', 'member'), may hold values from -6 to 6
- interp: bfloat16 [768, 128, 128], P('space'), may hold values from -0.25 to 0.25
- owner: int32 [768, 1], P('space'), may hold values from 0 to 7; in each aligned block of 96 rows (0 to 95, 96 to 191, ...) at most 24 rows name the same one
- local_block: int32 [768], P('space'), may hold values from 0 to 23
- ensemble: bfloat16 [40, 192, 64, 128], P('member', 'space'), may hold values from -6 to 6
- modes: float32 [64, 4], replicated, may hold values from -2 to 2
Outputs:
- applied_fine: float32 [768, 64, 128], P('space', 'member')
The draws below stay inside these ranges and needn't reach their ends.
Inputs may be any that keep to these rules, and one draw needn't show every extreme that they name: `owner`: among the rows of one device no value appears more than 24 times, and some value appears exactly 24 times.
All inputs are finite; a program needn't handle non-finite values.
Results may differ from the reference program's by a relative error of at most 0.0038.
Values may be sent and summed in bfloat16 or wider, within the bound.
No kernel may reach another device: no remote copies, remote signals or barrier semaphores. Data moves between devices by JAX's collectives and lax.ppermute only.
A program may use at most 64 MiB of HBM per device.

```python
import math
import jax
import jax.numpy as jnp
import numpy as np
from jax import lax

LEV = 64
MODES = 4
BW = 128
CBD = 24
FINE_DEV = 96
CAP = 24
CBLOCKS = 192
FBLOCKS = 768
MEMBERS = 40
N_SPACE = 8


def touch_ends(result, rng, low, high):
    dims = result.shape
    spot = [jax.random.randint(jax.random.fold_in(rng, axis), (), 0, dims[axis]) for axis in range(len(dims))]
    result = result.at[tuple(spot)].set(low)
    longest = dims.index(max(dims))
    spot[longest] = (spot[longest] + 1) % dims[longest]
    return result.at[tuple(spot)].set(high)


def block_levels(stream_key, dims, cuts, smallest, high):
    loudness, own = 1.0, jax.random.fold_in(stream_key, 6)
    for position, parts in cuts:
        draws = jnp.exp(jax.random.uniform(jax.random.fold_in(own, position), (parts,), jnp.float32, smallest / len(cuts), high / len(cuts)))
        loudness = loudness * jnp.repeat(draws, dims[position] // parts).reshape([-1 if axis == position else 1 for axis in range(len(dims))])
    return loudness


def deal_out(key, own, number, rows, count, top, bound, slope):
    order = jax.random.permutation(key, count)
    crowded, ordinary = load_shares(count, rows * top, bound, slope, True), load_shares(count, rows * top, bound, slope, False)
    places = jnp.arange(count)

    def named(lengths, turn):
        used = int((lengths > 0).sum())
        fixed = max(1, used // 4)
        shifted = fixed + (places - fixed + turn * (used - fixed)) % max(1, count - fixed)
        return jnp.zeros((count,), jnp.int32).at[order[jnp.where(places < fixed, places, shifted)]].set(jnp.asarray(lengths, jnp.int32))

    lengths = jnp.where(number % 4 == 0, named(crowded, number // 4), named(ordinary, number - number // 4 - 1))
    mixed = jax.random.permutation(jax.random.fold_in(own, 3), count)
    donor, sink = mixed[0:count // 2 * 2:2], mixed[1:count // 2 * 2:2]
    room = jnp.minimum(lengths[donor] - 1, bound - lengths[sink]) // 2
    room = jnp.where((donor == order[0]) | (sink == order[0]) | (lengths[sink] == 0), 0, jnp.maximum(room, 0))
    shifted = jax.random.randint(jax.random.fold_in(own, 4), (count // 2,), 0, 1 << 20) % (room + 1)
    lengths = lengths.at[donor].add(-shifted).at[sink].add(shifted)
    members = jnp.searchsorted(jnp.cumsum(lengths), jnp.arange(rows * top), side="right").astype(jnp.int32)
    listing = members.reshape(top, rows).T
    listing = listing[jax.random.permutation(jax.random.fold_in(own, 1), rows)]
    turn = jax.random.randint(jax.random.fold_in(own, 2), (rows, 1), 0, top)
    return jnp.take_along_axis(listing, (jnp.arange(top)[None, :] + turn) % top, axis=1)


def load_shares(amount, total, most, slope, full):
    weights = [(1 << 20) // math.isqrt(grade ** slope) + 1 for grade in range(1, amount + 1)]
    largest = most if full else min(most, max(-(-total // amount), total * weights[0] // sum(weights)))
    least = 1 if total - largest >= amount - 1 else 0
    counts, surplus = [largest] + [least] * (amount - 1), total - largest - least * (amount - 1)
    while surplus > 0:
        movable = [i for i in range(1, amount) if counts[i] < largest] or [i for i in range(1, amount) if counts[i] < most]
        pool, remaining = sum([weights[i] for i in movable]), surplus
        for i in movable:
            more = min(most - counts[i], max(1, remaining * weights[i] // pool), surplus)
            counts[i] = counts[i] + more
            surplus = surplus - more
    return np.array(counts)


def gaussian(rng, shape, width, reach, cuts=(), held_as=jnp.bfloat16):
    result = jax.random.normal(rng, shape, jnp.float32) * width
    if len(cuts) > 0:
        result = block_levels(rng, shape, cuts, -0.22, 0.18) * result
    return jnp.clip(result, min=-reach, max=reach).astype(held_as)


def setup_inputs(seed: int = 0) -> dict:
    key_list = jax.random.split(jax.random.key(seed), 7)
    increment = gaussian(key_list[0], (FBLOCKS, LEV, BW), 1.0, 6.0, ((0, 8), (1, 4)))
    interp = gaussian(key_list[1], (FBLOCKS, BW, BW), (4 * BW) ** -0.5, 0.25, ((0, 8),))
    owner_keys = jax.random.split(jax.random.fold_in(key_list[2], 1), FBLOCKS // FINE_DEV)
    owner_turns = jax.random.permutation(jax.random.fold_in(key_list[2], 3), FBLOCKS // FINE_DEV)
    owner = jax.vmap(lambda own, number: deal_out(jax.random.fold_in(key_list[2], 2), own, number, FINE_DEV, N_SPACE, 1, CAP, 2))(owner_keys, owner_turns).reshape((FBLOCKS, 1))
    local_block = touch_ends(jax.random.randint(key_list[3], (FBLOCKS,), 0, CBD), jax.random.fold_in(key_list[3], 1), 0, CBD - 1).astype(jnp.int32)
    ensemble = gaussian(key_list[4], (MEMBERS, CBLOCKS, LEV, BW), 1.0, 6.0, ((0, 4), (1, 8)))
    modes = gaussian(key_list[5], (LEV, MODES), 0.35, 2.0, (), jnp.float32)
    return {"increment": increment, "interp": interp, "owner": owner, "local_block": local_block, "ensemble": ensemble, "modes": modes}


def reference(increment, interp, owner, local_block, ensemble, modes):
    highest = lax.Precision.HIGHEST
    weights = interp.astype(jnp.float32)
    pieces = jnp.einsum("bli,bij->blj", increment.astype(jnp.float32), weights, precision=highest)
    target = (owner[:, 0] * CBD + local_block).astype(jnp.int32)
    restricted = jax.ops.segment_sum(pieces, target, num_segments=CBLOCKS).astype(jnp.bfloat16)
    restricted_wide = restricted.astype(jnp.float32)

    def member_step(total, member):
        values = member.astype(jnp.float32)
        schur = values * restricted_wide
        coefficients = jnp.einsum("clj,lk->ckj", schur, modes, precision=highest)
        rebuilt = jnp.einsum("ckj,lk->clj", coefficients, modes, precision=highest)
        return total + values * rebuilt, None

    start = jnp.zeros((CBLOCKS, LEV, BW), jnp.float32)
    total = lax.scan(member_step, start, ensemble)[0]
    applied = (total / (MEMBERS - 1)).astype(jnp.bfloat16)
    fine_values = applied[target].astype(jnp.float32)
    return jnp.einsum("blj,bij->bli", fine_values, weights, precision=highest)
```

```python
import functools

import jax
import jax.numpy as jnp
from jax import lax
from jax.experimental import pallas as pl
from jax.experimental.pallas import tpu as pltpu
from jax.sharding import PartitionSpec as P


F32, BF16 = jnp.float32, jnp.bfloat16
VM = pl.BlockSpec(memory_space=pltpu.VMEM)
SM = pl.BlockSpec(memory_space=pltpu.SMEM)
MIB = 1 << 20


def call(body, outs, specs, scratch, flops, nbytes, limit=24):
    return pl.pallas_call(
        body,
        out_shape=outs,
        in_specs=specs,
        out_specs=jax.tree.map(lambda _: VM, outs),
        scratch_shapes=scratch,
        compiler_params=pltpu.CompilerParams(vmem_limit_bytes=limit * MIB),
        cost_estimate=pl.CostEstimate(
            flops=flops, bytes_accessed=nbytes, transcendentals=0
        ),
    )


def restrict(increment, interp, owner, local_block, coarse, owners):
    fine, levels, width = increment.shape

    def body(own_ref, loc_ref, inc_ref, int_ref, self_ref, *rest):
        outs, acc = rest[:-1], rest[-1]
        me = lax.axis_index("space")
        acc[...] = jnp.zeros_like(acc)

        def step(b, carry):
            row = jnp.bitwise_xor(own_ref[b], me) * coarse + loc_ref[b]
            piece = jnp.dot(inc_ref[b], int_ref[b], preferred_element_type=F32)
            acc[row] += piece
            return carry

        lax.fori_loop(0, fine, step, 0, unroll=8)
        self_ref[...] = acc[pl.ds(0, coarse)]
        for k in range(1, owners):
            outs[k - 1][...] = acc[pl.ds(k * coarse, coarse)].astype(BF16)

    shape = (coarse, levels, width)
    outs = [jax.ShapeDtypeStruct(shape, F32)] + [
        jax.ShapeDtypeStruct(shape, BF16) for _ in range(1, owners)
    ]
    return call(
        body,
        outs,
        [SM, SM, VM, VM],
        [pltpu.VMEM((owners * coarse, levels, width), F32)],
        2 * fine * levels * width * width,
        2 * interp.size,
    )(owner, local_block, increment, interp)


def total_of(first, rest, dtype):
    def body(first_ref, *refs):
        total = first_ref[...]
        for ref in refs[:-1]:
            total = total + ref[...].astype(F32)
        refs[-1][...] = total.astype(dtype)

    return call(
        body,
        jax.ShapeDtypeStruct(first.shape, dtype),
        [VM] * (1 + len(rest)),
        [],
        first.size * len(rest),
        first.size * 2 * (len(rest) + 2),
    )(first, *rest)


def covariance(ensemble, modes, parts, scale):
    members, coarse, levels, width = ensemble.shape
    groups = len(parts)
    here = levels // groups
    kinds = modes.shape[1]

    def body(ens_ref, modes_ref, *refs):
        part_refs, self_ref = refs[:groups], refs[groups]
        outs = refs[groups + 1 : 2 * groups]
        rst, res = refs[2 * groups :]
        me = lax.axis_index("member")
        for k in range(groups):
            rst[jnp.bitwise_xor(me, k)] = part_refs[k][...].astype(F32)
        m_full = modes_ref[...]
        m_high = m_full.astype(BF16).astype(F32)
        m_low = m_full - m_high
        spread = jnp.concatenate([m_high, m_high, m_low, m_low], axis=1)
        back = spread.astype(BF16)
        high_t = jnp.concatenate([m_high] * 4, axis=1).T
        low_t = jnp.concatenate([m_low] * 4, axis=1).T
        gather = jnp.concatenate([high_t, high_t, low_t], axis=1).astype(BF16)
        row = lax.broadcasted_iota(jnp.int32, (4 * kinds, 2 * width), 0)
        takes_low = (row // kinds) % 2 == 1

        def step(c, carry):
            weight = rst[:, c].reshape(levels, width)
            wide = jnp.concatenate([weight, weight], axis=1)
            total = None
            for m in range(0, members, 2):
                pair = jnp.concatenate([ens_ref[m, c], ens_ref[m + 1, c]], axis=1)
                values = pair.astype(F32)
                schur = values * wide
                high = schur.astype(BF16)
                low = (schur - high.astype(F32)).astype(BF16)
                stack = jnp.concatenate([high, low, high], axis=0)
                coeff = jnp.dot(gather, stack, preferred_element_type=F32)
                c_high = coeff.astype(BF16).astype(F32)
                mixed = jnp.where(takes_low, coeff - c_high, c_high).astype(BF16)
                local = jnp.dot(back, mixed, preferred_element_type=F32)
                term = values * local
                total = term if total is None else total + term
            both = (total[:, :width] + total[:, width:]) * scale
            res[:, c] = both.reshape(groups, here, width)
            return carry

        lax.fori_loop(0, coarse, step, 0, unroll=2)
        self_ref[...] = res[me]
        for k in range(1, groups):
            outs[k - 1][...] = res[jnp.bitwise_xor(me, k)].astype(BF16)

    shape = (coarse, here, width)
    outs = [jax.ShapeDtypeStruct(shape, F32)] + [
        jax.ShapeDtypeStruct(shape, BF16) for _ in range(1, groups)
    ]
    return call(
        body,
        outs,
        [VM] * (2 + groups),
        [pltpu.VMEM((groups,) + shape, F32), pltpu.VMEM((groups,) + shape, F32)],
        ensemble.size * 64,
        ensemble.size * 2,
    )(ensemble, modes, *parts)


def expand(pieces, interp, owner, local_block):
    owners = len(pieces)
    coarse, levels, width = pieces[0].shape
    fine = interp.shape[0]

    def body(own_ref, loc_ref, int_ref, *refs):
        out_ref, table = refs[-2:]
        me = lax.axis_index("space")
        for k in range(owners):
            table[pl.ds(k * coarse, coarse)] = refs[k][...]

        def step(b, carry):
            row = jnp.bitwise_xor(own_ref[b], me) * coarse + loc_ref[b]
            out_ref[b] = lax.dot_general(
                table[row],
                int_ref[b],
                (((1,), (1,)), ((), ())),
                preferred_element_type=F32,
            )
            return carry

        lax.fori_loop(0, fine, step, 0, unroll=8)

    return call(
        body,
        jax.ShapeDtypeStruct((fine, levels, width), F32),
        [SM, SM, VM] + [VM] * owners,
        [pltpu.VMEM((owners * coarse, levels, width), BF16)],
        2 * fine * levels * width * width,
        2 * interp.size,
    )(owner, local_block, interp, *pieces)


def swap(value, axis, size, k):
    return lax.ppermute(value, axis, [(i, i ^ k) for i in range(size)])


def on_device(increment, interp, owner, local_block, ensemble, modes):
    owners = lax.axis_size("space")
    groups = lax.axis_size("member")
    coarse = ensemble.shape[1]
    owner = owner.reshape(-1)
    inner = 1 << ((owners.bit_length() - 1) // 2)

    mine, *sends = restrict(increment, interp, owner, local_block, coarse, owners)
    arrived = [swap(v, "space", owners, k + 1) for k, v in enumerate(sends)]
    restricted = total_of(mine, arrived, F32)
    parts = [restricted] + [
        swap(restricted, "member", groups, k) for k in range(1, groups)
    ]
    scale = 1.0 / (ensemble.shape[0] * groups - 1)
    mine, *sends = covariance(ensemble, modes, parts, scale)
    arrived = [swap(v, "member", groups, k + 1) for k, v in enumerate(sends)]
    applied = total_of(mine, arrived, BF16)
    line = [applied] + [
        swap(applied, "space", owners, k * inner) for k in range(1, owners // inner)
    ]
    pieces = []
    for value in line:
        pieces.append(value)
        for k in range(1, inner):
            pieces.append(swap(value, "space", owners, k))
    return expand(pieces, interp, owner, local_block)


def solution(mesh):
    in_specs = (
        P("space", "member", None),
        P("space", None, None),
        P("space", None),
        P("space"),
        P("member", "space", None, None),
        P(),
    )
    out_specs = P("space", "member", None)
    return jax.shard_map(
        on_device, mesh=mesh, in_specs=in_specs, out_specs=out_specs, check_vma=False
    )
```

```python
import functools

import jax
import jax.numpy as jnp
from jax import lax
from jax.experimental import pallas as pl
from jax.experimental.pallas import tpu as pltpu
from jax.sharding import PartitionSpec as P


F32, BF16 = jnp.float32, jnp.bfloat16
VM = pl.BlockSpec(memory_space=pltpu.VMEM)
SM = pl.BlockSpec(memory_space=pltpu.SMEM)
HB = pl.BlockSpec(memory_space=pltpu.HBM)
MIB = 1 << 20


def call(body, outs, specs, scratch, flops, nbytes, limit=24):
    return pl.pallas_call(
        body,
        out_shape=outs,
        in_specs=specs,
        out_specs=jax.tree.map(lambda _: VM, outs),
        scratch_shapes=scratch,
        compiler_params=pltpu.CompilerParams(vmem_limit_bytes=limit * MIB),
        cost_estimate=pl.CostEstimate(
            flops=flops, bytes_accessed=nbytes, transcendentals=0
        ),
    )


def restrict(increment, interp, owner, local_block, coarse, owners):
    fine, levels, width = increment.shape
    chunks = 4 if fine % 32 == 0 else 1
    part = fine // chunks

    def body(own_hbm, loc_hbm, inc_hbm, int_hbm, self_ref, *rest):
        outs = rest[: owners - 1]
        own_ref, loc_ref, inc_ref, int_ref, acc, sems = rest[owners - 1 :]
        me = lax.axis_index("space")

        def copy(src, dst, i, sem):
            at = pl.ds(i * part, part)
            return pltpu.make_async_copy(src.at[at], dst.at[at], sems.at[sem])

        small = [
            pltpu.make_async_copy(own_hbm, own_ref, sems.at[0]),
            pltpu.make_async_copy(loc_hbm, loc_ref, sems.at[1]),
        ]
        large = [
            (copy(inc_hbm, inc_ref, i, 2 + 2 * i), copy(int_hbm, int_ref, i, 3 + 2 * i))
            for i in range(chunks)
        ]
        for cp in small:
            cp.start()
        for pair in large:
            pair[0].start()
            pair[1].start()
        acc[...] = jnp.zeros_like(acc)
        for cp in small:
            cp.wait()

        def step(b, carry):
            row = jnp.bitwise_xor(own_ref[b], me) * coarse + loc_ref[b]
            piece = jnp.dot(inc_ref[b], int_ref[b], preferred_element_type=F32)
            acc[row] += piece
            return carry

        for i, pair in enumerate(large):
            pair[0].wait()
            pair[1].wait()
            lax.fori_loop(i * part, (i + 1) * part, step, 0, unroll=8)
        self_ref[...] = acc[pl.ds(0, coarse)]
        for k in range(1, owners):
            outs[k - 1][...] = acc[pl.ds(k * coarse, coarse)].astype(BF16)

    shape = (coarse, levels, width)
    outs = [jax.ShapeDtypeStruct(shape, F32)] + [
        jax.ShapeDtypeStruct(shape, BF16) for _ in range(1, owners)
    ]
    return call(
        body,
        outs,
        [HB] * 4,
        [
            pltpu.SMEM(owner.shape, owner.dtype),
            pltpu.SMEM(local_block.shape, local_block.dtype),
            pltpu.VMEM(increment.shape, BF16),
            pltpu.VMEM(interp.shape, BF16),
            pltpu.VMEM((owners * coarse, levels, width), F32),
            pltpu.SemaphoreType.DMA((2 + 2 * chunks,)),
        ],
        2 * fine * levels * width * width,
        2 * interp.size,
    )(owner, local_block, increment, interp)


def transposed(interp):
    fine = interp.shape[0]

    def body(int_ref, out_ref):
        def step(b, carry):
            out_ref[b] = int_ref[b].T
            return carry

        lax.fori_loop(0, fine, step, 0, unroll=8)

    return call(
        body,
        jax.ShapeDtypeStruct(interp.shape, interp.dtype),
        [VM],
        [],
        64 * interp.size,
        4 * interp.size,
    )(interp)


def total_of(first, rest, dtype):
    def body(first_ref, *refs):
        total = first_ref[...]
        for ref in refs[:-1]:
            total = total + ref[...].astype(F32)
        refs[-1][...] = total.astype(dtype)

    return call(
        body,
        jax.ShapeDtypeStruct(first.shape, dtype),
        [VM] * (1 + len(rest)),
        [],
        first.size * len(rest),
        first.size * 2 * (len(rest) + 2),
    )(first, *rest)


def covariance(ensemble, modes, parts, scale):
    members, coarse, levels, width = ensemble.shape
    groups = len(parts)
    here = levels // groups
    kinds = modes.shape[0]
    rows = 4 * kinds
    chunks = 4 if coarse % 4 == 0 else 1
    part = coarse // chunks

    def body(ens_hbm, modes_ref, *refs):
        part_refs, self_ref = refs[:groups], refs[groups]
        outs = refs[groups + 1 : 2 * groups]
        ens_ref, rst, res, mix, sems = refs[2 * groups :]
        me = lax.axis_index("member")

        def copy(i):
            at = pl.ds(i * part, part)
            return pltpu.make_async_copy(
                ens_hbm.at[:, at], ens_ref.at[:, at], sems.at[i]
            )

        for i in range(chunks):
            copy(i).start()
        for k in range(groups):
            rst[jnp.bitwise_xor(me, k)] = part_refs[k][...].astype(F32)
        full = modes_ref[...]
        high = full.astype(BF16).astype(F32)
        low = full - high
        back = jnp.concatenate([high, high, low, low], axis=0).T.astype(BF16)
        tall = jnp.concatenate([high] * 4 + [low] * 4, axis=0)
        gather = jnp.concatenate([tall, tall], axis=1).astype(BF16)
        row = lax.broadcasted_iota(jnp.int32, (rows, members * width), 0)
        takes_low = (row // kinds) % 2 == 1

        def first(c):
            weight = rst[:, c].reshape(levels, width)
            highs, lows = [], []
            for m in range(members):
                schur = ens_ref[m, c].astype(F32) * weight
                top = schur.astype(BF16)
                highs.append(top)
                lows.append((schur - top.astype(F32)).astype(BF16))
            stack = jnp.concatenate(
                [jnp.concatenate(highs, axis=1), jnp.concatenate(lows, axis=1)], axis=0
            )
            both = jnp.dot(gather, stack, preferred_element_type=F32)
            coeff = both[:rows] + both[rows:]
            top = coeff.astype(BF16).astype(F32)
            mix[c] = jnp.where(takes_low, coeff - top, top).astype(BF16)

        def second(c):
            local = jnp.dot(back, mix[c], preferred_element_type=F32)
            total = None
            for m in range(members):
                at = slice(m * width, (m + 1) * width)
                term = ens_ref[m, c].astype(F32) * local[:, at]
                total = term if total is None else total + term
            res[:, c] = (total * scale).reshape(groups, here, width)

        def phase_one(i, carry):
            copy(i).wait()
            for j in range(part):
                first(i * part + j)
            return carry

        def phase_two(i, carry):
            for j in range(part):
                second(i * part + j)
            return carry

        lax.fori_loop(0, chunks, phase_one, 0)
        lax.fori_loop(0, chunks, phase_two, 0)
        self_ref[...] = res[me]
        for k in range(1, groups):
            outs[k - 1][...] = res[jnp.bitwise_xor(me, k)].astype(BF16)

    shape = (coarse, here, width)
    outs = [jax.ShapeDtypeStruct(shape, F32)] + [
        jax.ShapeDtypeStruct(shape, BF16) for _ in range(1, groups)
    ]
    return call(
        body,
        outs,
        [HB] + [VM] * (1 + groups),
        [
            pltpu.VMEM(ensemble.shape, BF16),
            pltpu.VMEM((groups,) + shape, F32),
            pltpu.VMEM((groups,) + shape, F32),
            pltpu.VMEM((coarse, rows, members * width), BF16),
            pltpu.SemaphoreType.DMA((chunks,)),
        ],
        ensemble.size * 64,
        ensemble.size * 2,
    )(ensemble, modes, *parts)


def expand(pieces, interp, owner, local_block):
    owners = len(pieces)
    coarse, levels, width = pieces[0].shape
    fine = interp.shape[0]

    def body(own_ref, loc_ref, int_ref, *refs):
        out_ref, table = refs[-2:]
        me = lax.axis_index("space")
        for k in range(owners):
            table[pl.ds(k * coarse, coarse)] = refs[k][...]

        def step(b, carry):
            row = jnp.bitwise_xor(own_ref[b], me) * coarse + loc_ref[b]
            out_ref[b] = jnp.dot(table[row], int_ref[b], preferred_element_type=F32)
            return carry

        lax.fori_loop(0, fine, step, 0, unroll=8)

    return call(
        body,
        jax.ShapeDtypeStruct((fine, levels, width), F32),
        [SM, SM, VM] + [VM] * owners,
        [pltpu.VMEM((owners * coarse, levels, width), BF16)],
        2 * fine * levels * width * width,
        2 * interp.size,
    )(owner, local_block, interp, *pieces)


def swap(value, axis, size, k):
    return lax.ppermute(value, axis, [(i, i ^ k) for i in range(size)])


def on_device(increment, interp, owner, local_block, ensemble, modes):
    owners = lax.axis_size("space")
    groups = lax.axis_size("member")
    coarse = ensemble.shape[1]
    owner = owner.reshape(-1)
    inner = 1 << ((owners.bit_length() - 1) // 2)

    mine, *sends = restrict(increment, interp, owner, local_block, coarse, owners)
    arrived = [swap(v, "space", owners, k + 1) for k, v in enumerate(sends)]
    flipped = transposed(interp)
    restricted = total_of(mine, arrived, F32)
    parts = [restricted]
    step = groups // 2
    while step:
        parts = parts + [swap(v, "member", groups, step) for v in parts]
        step //= 2
    order = [0]
    step = groups // 2
    while step:
        order = order + [v ^ step for v in order]
        step //= 2
    parts = [parts[order.index(k)] for k in range(groups)]
    scale = 1.0 / (ensemble.shape[0] * groups - 1)
    mine, *sends = covariance(ensemble, modes.T, parts, scale)
    arrived = [swap(v, "member", groups, k + 1) for k, v in enumerate(sends)]
    applied = total_of(mine, arrived, BF16)
    line = [applied] + [
        swap(applied, "space", owners, k * inner) for k in range(1, owners // inner)
    ]
    pieces = []
    for i, value in enumerate(line):
        pieces.append(value)
        for k in range(1, inner):
            if i == 1:
                pieces.append(swap(applied, "space", owners, i * inner + k))
            else:
                pieces.append(swap(value, "space", owners, k))
    return expand(pieces, flipped, owner, local_block)


def solution(mesh):
    in_specs = (
        P("space", "member", None),
        P("space", None, None),
        P("space", None),
        P("space"),
        P("member", "space", None, None),
        P(),
    )
    out_specs = P("space", "member", None)
    return jax.shard_map(
        on_device, mesh=mesh, in_specs=in_specs, out_specs=out_specs, check_vma=False
    )
```

```python
import jax
import jax.numpy as jnp
from jax import lax
from jax.experimental import pallas as pl
from jax.experimental.pallas import tpu as pltpu
from jax.sharding import PartitionSpec as P


F32, BF16 = jnp.float32, jnp.bfloat16
VM = pl.BlockSpec(memory_space=pltpu.VMEM)
SM = pl.BlockSpec(memory_space=pltpu.SMEM)
HB = pl.BlockSpec(memory_space=pltpu.HBM)
MIB = 1 << 20


def call(body, outs, specs, scratch, flops, nbytes, limit=24):
    return pl.pallas_call(
        body,
        out_shape=outs,
        in_specs=specs,
        out_specs=jax.tree.map(lambda _: VM, outs),
        scratch_shapes=scratch,
        compiler_params=pltpu.CompilerParams(vmem_limit_bytes=int(limit * MIB)),
        cost_estimate=pl.CostEstimate(
            flops=flops, bytes_accessed=nbytes, transcendentals=0
        ),
    )


def two_dots(left, right, blocks, b):
    levels, width = left.shape
    both = jnp.dot(
        jnp.concatenate([left, right], axis=0),
        jnp.concatenate([blocks[b], blocks[b + 1]], axis=1),
        preferred_element_type=F32,
    )
    return [both[:levels, :width], both[levels:, width:]]


def restrict(increment, interp, target, plan, coarse, owners, inner):
    fine, levels, width = increment.shape
    chunks = 4 if fine % 32 == 0 else 1
    part = fine // chunks
    outs, fills = [], []
    for start, count, staged in plan:
        for k in range(inner if staged else owners):
            offsets = range(k, owners, inner) if staged else (k,)
            dtype = BF16 if k else F32
            shape = (count * len(offsets), levels, width)
            outs.append(jax.ShapeDtypeStruct(shape, dtype))
            fills.append((start, count, offsets, dtype))

    def body(row_ref, inc_hbm, int_hbm, *rest):
        out_refs = rest[: len(outs)]
        inc_ref, int_ref, acc, sems = rest[len(outs) :]
        me = lax.axis_index("space")

        def copy(src, dst, i, sem):
            at = pl.ds(i * part, part)
            return pltpu.make_async_copy(src.at[at], dst.at[at], sems.at[sem])

        large = [
            (copy(inc_hbm, inc_ref, i, 2 * i), copy(int_hbm, int_ref, i, 2 * i + 1))
            for i in range(chunks)
        ]
        for pair in large:
            pair[0].start()
            pair[1].start()
        acc[...] = jnp.zeros_like(acc)
        for i, pair in enumerate(large):
            pair[0].wait()
            pair[1].wait()
            values = []
            for b in range(i * part, (i + 1) * part, 2):
                values += two_dots(inc_ref[b], inc_ref[b + 1], int_ref, b)
            for j, value in enumerate(values):
                acc[row_ref[i * part + j]] += value
        for ref, (start, count, offsets, dtype) in zip(out_refs, fills):
            for i, k in enumerate(offsets):
                at = jnp.bitwise_xor(me, k) * coarse + start
                value = acc[pl.ds(at, count)]
                ref[pl.ds(i * count, count)] = value.astype(dtype)

    return call(
        body,
        outs,
        [SM, HB, HB],
        [
            pltpu.VMEM(increment.shape, BF16),
            pltpu.VMEM(interp.shape, BF16),
            pltpu.VMEM((owners * coarse, levels, width), F32),
            pltpu.SemaphoreType.DMA((2 * chunks,)),
        ],
        2 * fine * levels * width * width,
        2 * interp.size,
        RESTRICT_MIB,
    )(target, increment, interp)


def staged_total(first, rest, outer):
    count = first.shape[0] // outer
    shape = (count,) + first.shape[1:]

    def body(first_ref, *refs):
        ins, outs = refs[: len(rest)], refs[len(rest) :]
        for i, out in enumerate(outs):
            at = pl.ds(i * count, count)
            total = first_ref[at]
            for ref in ins:
                total = total + ref[at].astype(F32)
            out[...] = total.astype(out.dtype)

    return call(
        body,
        [jax.ShapeDtypeStruct(shape, BF16 if i else F32) for i in range(outer)],
        [VM] * (1 + len(rest)),
        [],
        first.size * len(rest),
        first.size * 2 * (len(rest) + 2),
    )(first, *rest)


def transposed(interp):
    fine = interp.shape[0]

    def body(int_ref, out_ref):
        def step(b, carry):
            out_ref[b] = int_ref[b].T
            return carry

        lax.fori_loop(0, fine, step, 0, unroll=8)

    return call(
        body,
        jax.ShapeDtypeStruct(interp.shape, interp.dtype),
        [VM],
        [],
        64 * interp.size,
        4 * interp.size,
    )(interp)


def total_of(sets, dtype):
    counts = [first.shape[0] for first, _ in sets]
    flat = [v for first, rest in sets for v in (first, *rest)]

    def body(*refs):
        out, refs, start = refs[-1], refs[:-1], 0
        for (_, rest), count in zip(sets, counts):
            total = refs[0][...]
            for ref in refs[1 : 1 + len(rest)]:
                total = total + ref[...].astype(F32)
            out[pl.ds(start, count)] = total.astype(dtype)
            refs, start = refs[1 + len(rest) :], start + count

    shape = (sum(counts),) + flat[0].shape[1:]
    size = sum(v.size for v in flat)
    return call(
        body, jax.ShapeDtypeStruct(shape, dtype), [VM] * len(flat), [], size, 2 * size
    )(*flat)


def covariance(ensemble, modes, parts, scale):
    members, _, levels, width = ensemble.shape
    coarse = parts[0].shape[0]
    groups = len(parts)
    here = levels // groups
    kinds = modes.shape[0]
    rows = 4 * kinds
    chunks = 4 if coarse % 4 == 0 else 1
    part = coarse // chunks

    def body(ens_hbm, modes_ref, *refs):
        part_refs, self_ref = refs[:groups], refs[groups]
        outs = refs[groups + 1 : 2 * groups]
        ens_ref, rst, res, mix, sems = refs[2 * groups :]
        me = lax.axis_index("member")

        def copy(i):
            at = pl.ds(i * part, part)
            return pltpu.make_async_copy(
                ens_hbm.at[:, at], ens_ref.at[:, at], sems.at[i]
            )

        for i in range(chunks):
            copy(i).start()
        for k in range(groups):
            rst[jnp.bitwise_xor(me, k)] = part_refs[k][...].astype(F32)
        full = modes_ref[...]
        high = full.astype(BF16).astype(F32)
        low = full - high
        back = jnp.concatenate([high, high, low, low], axis=0).T.astype(BF16)
        tall = jnp.concatenate([high] * 4 + [low] * 4, axis=0)
        gather = jnp.concatenate([tall, tall], axis=1).astype(BF16)
        row = lax.broadcasted_iota(jnp.int32, (rows, members * width), 0)
        takes_low = (row // kinds) % 2 == 1

        def first(c):
            weight = rst[:, c].reshape(levels, width)
            highs, lows = [], []
            for m in range(members):
                schur = ens_ref[m, c].astype(F32) * weight
                top = schur.astype(BF16)
                highs.append(top)
                lows.append((schur - top.astype(F32)).astype(BF16))
            stack = jnp.concatenate(
                [jnp.concatenate(highs, axis=1), jnp.concatenate(lows, axis=1)], axis=0
            )
            both = jnp.dot(gather, stack, preferred_element_type=F32)
            coeff = both[:rows] + both[rows:]
            top = coeff.astype(BF16).astype(F32)
            mix[c] = jnp.where(takes_low, coeff - top, top).astype(BF16)

        def second(c):
            local = jnp.dot(back, mix[c], preferred_element_type=F32)
            total = None
            for m in range(members):
                at = slice(m * width, (m + 1) * width)
                term = ens_ref[m, c].astype(F32) * local[:, at]
                total = term if total is None else total + term
            res[:, c] = (total * scale).reshape(groups, here, width)

        def phase_one(i, carry):
            copy(i).wait()
            for j in range(part):
                first(i * part + j)
            return carry

        def phase_two(i, carry):
            for j in range(part):
                second(i * part + j)
            return carry

        lax.fori_loop(0, chunks, phase_one, 0)
        lax.fori_loop(0, chunks, phase_two, 0)
        self_ref[...] = res[me]
        for k in range(1, groups):
            outs[k - 1][...] = res[jnp.bitwise_xor(me, k)].astype(BF16)

    shape = (coarse, here, width)
    outs = [jax.ShapeDtypeStruct(shape, F32)] + [
        jax.ShapeDtypeStruct(shape, BF16) for _ in range(1, groups)
    ]
    return call(
        body,
        outs,
        [HB] + [VM] * (1 + groups),
        [
            pltpu.VMEM(ensemble.shape, BF16),
            pltpu.VMEM((groups,) + shape, F32),
            pltpu.VMEM((groups,) + shape, F32),
            pltpu.VMEM((coarse, rows, members * width), BF16),
            pltpu.SemaphoreType.DMA((chunks,)),
        ],
        members * parts[0].size * groups * 64,
        members * parts[0].size * groups * 2,
    )(ensemble, modes, *parts)


def expand(pieces, interp, target):
    owners = len(pieces)
    coarse, levels, width = pieces[0].shape
    fine = interp.shape[0]

    def body(row_ref, int_ref, *refs):
        out_ref, table = refs[-2:]
        me = lax.axis_index("space")
        for k in range(owners):
            at = jnp.bitwise_xor(me, k) * coarse
            table[pl.ds(at, coarse)] = refs[k][...]

        def step(p, carry):
            b = 2 * p
            pair = two_dots(table[row_ref[b]], table[row_ref[b + 1]], int_ref, b)
            out_ref[b], out_ref[b + 1] = pair
            return carry

        lax.fori_loop(0, fine // 2, step, 0, unroll=12)

    return call(
        body,
        jax.ShapeDtypeStruct((fine, levels, width), F32),
        [SM, VM] + [VM] * owners,
        [pltpu.VMEM((owners * coarse, levels, width), BF16)],
        2 * fine * levels * width * width,
        2 * interp.size,
    )(target, interp, *pieces)


def swap(value, axis, size, k):
    return lax.ppermute(value, axis, [(i, i ^ k) for i in range(size)])


def gather_members(value, groups):
    parts, order = [value], [0]
    step = groups // 2
    while step:
        parts = parts + [swap(v, "member", groups, step) for v in parts]
        order = order + [v ^ step for v in order]
        step //= 2
    return [parts[order.index(k)] for k in range(groups)]


def gather_space(value, owners, inner):
    outer = owners // inner

    def send(part, k):
        return swap(part, "space", owners, k)

    pieces = {0: value}
    for i in reversed(range(2, outer)):
        pieces[i * inner] = send(value, i * inner)
    for k in range(1, inner):
        pieces[inner + k] = send(value, inner + k)
    pieces[inner] = send(value, inner)
    for k in range(1, inner):
        pieces[k] = send(value, k)
    for i in reversed(range(2, outer)):
        for k in range(1, inner):
            pieces[i * inner + k] = send(pieces[i * inner], k)
    return [pieces[k] for k in range(owners)]


DIRECT = 0.5
RESTRICT_MIB = 52


def on_device(increment, interp, owner, local_block, ensemble, modes):
    owners = lax.axis_size("space")
    groups = lax.axis_size("member")
    coarse = ensemble.shape[1]
    target = owner.reshape(-1) * coarse + local_block
    inner = 1 << ((owners.bit_length() - 1) // 2)
    outer = owners // inner
    cut = int(coarse * DIRECT)
    plan = [(0, cut, False), (cut, coarse - cut, True)]
    plan = [entry for entry in plan if entry[1]]
    scale = 1.0 / (ensemble.shape[0] * groups - 1)

    sums = restrict(increment, interp, target, plan, coarse, owners, inner)
    flipped = transposed(interp)
    direct, staged = (sums[:owners], sums[owners:]) if cut else ([], sums)

    def send(value, k):
        return swap(value, "space", owners, k)

    sets, near, arrived, second = [], [], {}, {}
    if staged:
        near = [send(v, k + 1) for k, v in enumerate(staged[1:])]
    if direct:
        for k in range(owners // 2, owners):
            arrived[k] = send(direct[k], k)
    if staged:
        mine, *sends = staged_total(staged[0], near, outer)
        for i in reversed(range(1, outer)):
            second[i] = send(sends[i - 1], i * inner)
    if direct:
        for k in reversed(range(1, owners // 2)):
            arrived[k] = send(direct[k], k)
        sets.append((direct[0], [arrived[k] for k in range(1, owners)]))
    if staged:
        sets.append((mine, [second[i] for i in range(1, outer)]))
    restricted = total_of(sets, F32)
    parts = gather_members(restricted, groups)
    mine, *sends = covariance(ensemble, modes.T, parts, scale)
    arrived = [swap(v, "member", groups, k + 1) for k, v in enumerate(sends)]
    applied = total_of([(mine, arrived)], BF16)
    pieces = gather_space(applied, owners, inner)
    return expand(pieces, flipped, target)


def solution(mesh):
    in_specs = (
        P("space", "member", None),
        P("space", None, None),
        P("space", None),
        P("space"),
        P("member", "space", None, None),
        P(),
    )
    out_specs = P("space", "member", None)

    return jax.shard_map(
        on_device, mesh=mesh, in_specs=in_specs, out_specs=out_specs, check_vma=False
    )
```

```python
import jax
import jax.numpy as jnp
from jax import lax
from jax.experimental import pallas as pl
from jax.experimental.pallas import tpu as pltpu
from jax.sharding import PartitionSpec as P


F32, BF16 = jnp.float32, jnp.bfloat16
VM = pl.BlockSpec(memory_space=pltpu.VMEM)
SM = pl.BlockSpec(memory_space=pltpu.SMEM)
HB = pl.BlockSpec(memory_space=pltpu.HBM)
MIB = 1 << 20


def call(body, outs, specs, scratch, flops, nbytes, limit=24):
    return pl.pallas_call(
        body,
        out_shape=outs,
        in_specs=specs,
        out_specs=jax.tree.map(lambda _: VM, outs),
        scratch_shapes=scratch,
        compiler_params=pltpu.CompilerParams(vmem_limit_bytes=int(limit * MIB)),
        cost_estimate=pl.CostEstimate(
            flops=flops, bytes_accessed=nbytes, transcendentals=0
        ),
    )


def two_dots(left, right, blocks, b):
    levels, width = left.shape
    both = jnp.dot(
        jnp.concatenate([left, right], axis=0),
        jnp.concatenate([blocks[b], blocks[b + 1]], axis=1),
        preferred_element_type=F32,
    )
    return [both[:levels, :width], both[levels:, width:]]


def restrict(increment, interp, target, plan, coarse, owners, inner):
    fine, levels, width = increment.shape
    chunks = 4 if fine % 32 == 0 else 1
    part = fine // chunks
    outs, fills = [], []
    for start, count, staged in plan:
        for k in range(inner if staged else owners):
            offsets = range(k, owners, inner) if staged else (k,)
            dtype = BF16 if k else F32
            shape = (count * len(offsets), levels, width)
            outs.append(jax.ShapeDtypeStruct(shape, dtype))
            fills.append((start, count, offsets, dtype))

    def body(row_ref, inc_hbm, int_hbm, *rest):
        out_refs = rest[: len(outs)]
        inc_ref, int_ref, acc, sems = rest[len(outs) :]
        me = lax.axis_index("space")

        def copy(src, dst, i, sem):
            at = pl.ds(i * part, part)
            return pltpu.make_async_copy(src.at[at], dst.at[at], sems.at[sem])

        large = [
            (copy(inc_hbm, inc_ref, i, 2 * i), copy(int_hbm, int_ref, i, 2 * i + 1))
            for i in range(chunks)
        ]
        for pair in large:
            pair[0].start()
            pair[1].start()
        acc[...] = jnp.zeros_like(acc)
        for i, pair in enumerate(large):
            pair[0].wait()
            pair[1].wait()
            values = []
            for b in range(i * part, (i + 1) * part, 2):
                values += two_dots(inc_ref[b], inc_ref[b + 1], int_ref, b)
            for j, value in enumerate(values):
                acc[row_ref[i * part + j]] += value
        for ref, (start, count, offsets, dtype) in zip(out_refs, fills):
            for i, k in enumerate(offsets):
                at = jnp.bitwise_xor(me, k) * coarse + start
                value = acc[pl.ds(at, count)]
                ref[pl.ds(i * count, count)] = value.astype(dtype)

    return call(
        body,
        outs,
        [SM, HB, HB],
        [
            pltpu.VMEM(increment.shape, BF16),
            pltpu.VMEM(interp.shape, BF16),
            pltpu.VMEM((owners * coarse, levels, width), F32),
            pltpu.SemaphoreType.DMA((2 * chunks,)),
        ],
        2 * fine * levels * width * width,
        2 * interp.size,
        RESTRICT_MIB,
    )(target, increment, interp)


def staged_total(sets, outer):
    counts = [first.shape[0] // outer for first, _ in sets]
    flat = [v for first, rest in sets for v in (first, *rest)]
    shape = (sum(counts),) + flat[0].shape[1:]

    def body(*refs):
        ins, outs = refs[: len(flat)], refs[len(flat) :]
        start = 0
        for (_, rest), count in zip(sets, counts):
            for i, out in enumerate(outs):
                at = pl.ds(i * count, count)
                total = ins[0][at]
                for ref in ins[1 : 1 + len(rest)]:
                    total = total + ref[at].astype(F32)
                out[pl.ds(start, count)] = total.astype(out.dtype)
            ins, start = ins[1 + len(rest) :], start + count

    size = sum(v.size for v in flat)
    return call(
        body,
        [jax.ShapeDtypeStruct(shape, BF16 if i else F32) for i in range(outer)],
        [VM] * len(flat),
        [],
        size,
        2 * size,
    )(*flat)


def transposed(interp):
    fine = interp.shape[0]

    def body(int_ref, out_ref):
        def step(b, carry):
            out_ref[b] = int_ref[b].T
            return carry

        lax.fori_loop(0, fine, step, 0, unroll=8)

    return call(
        body,
        jax.ShapeDtypeStruct(interp.shape, interp.dtype),
        [VM],
        [],
        64 * interp.size,
        4 * interp.size,
    )(interp)


def total_of(sets, dtype):
    counts = [first.shape[0] for first, _ in sets]
    flat = [v for first, rest in sets for v in (first, *rest)]

    def body(*refs):
        out, refs, start = refs[-1], refs[:-1], 0
        for (_, rest), count in zip(sets, counts):
            total = refs[0][...]
            for ref in refs[1 : 1 + len(rest)]:
                total = total + ref[...].astype(F32)
            out[pl.ds(start, count)] = total.astype(dtype)
            refs, start = refs[1 + len(rest) :], start + count

    shape = (sum(counts),) + flat[0].shape[1:]
    size = sum(v.size for v in flat)
    return call(
        body, jax.ShapeDtypeStruct(shape, dtype), [VM] * len(flat), [], size, 2 * size
    )(*flat)


def covariance(ensemble, modes, parts, scale, start):
    members, _, levels, width = ensemble.shape
    coarse = parts[0].shape[0]
    groups = len(parts)
    here = levels // groups
    kinds = modes.shape[0]
    rows = 4 * kinds
    chunks = next(n for n in (4, 2, 1) if coarse % n == 0 and coarse // n > 3 or n == 1)
    part = coarse // chunks

    def body(ens_hbm, modes_ref, *refs):
        part_refs, outs = refs[:groups], refs[groups : groups + 2]
        ens_ref, rst, res, mix, sems = refs[groups + 2 :]
        me = lax.axis_index("member")

        def copy(i):
            here_at = pl.ds(i * part, part)
            there_at = pl.ds(start + i * part, part)
            return pltpu.make_async_copy(
                ens_hbm.at[:, there_at], ens_ref.at[:, here_at], sems.at[i]
            )

        for i in range(chunks):
            copy(i).start()
        for k in range(groups):
            rst[jnp.bitwise_xor(me, k)] = part_refs[k][...].astype(F32)
        full = modes_ref[...]
        high = full.astype(BF16).astype(F32)
        low = full - high
        back = jnp.concatenate([high, high, low, low], axis=0).T.astype(BF16)
        tall = jnp.concatenate([high] * 4 + [low] * 4, axis=0)
        gather = jnp.concatenate([tall, tall], axis=1).astype(BF16)
        row = lax.broadcasted_iota(jnp.int32, (rows, members * width), 0)
        takes_low = (row // kinds) % 2 == 1

        def first(c):
            weight = rst[:, c].reshape(levels, width)
            highs, lows = [], []
            for m in range(members):
                schur = ens_ref[m, c].astype(F32) * weight
                top = schur.astype(BF16)
                highs.append(top)
                lows.append((schur - top.astype(F32)).astype(BF16))
            stack = jnp.concatenate(
                [jnp.concatenate(highs, axis=1), jnp.concatenate(lows, axis=1)], axis=0
            )
            both = jnp.dot(gather, stack, preferred_element_type=F32)
            coeff = both[:rows] + both[rows:]
            top = coeff.astype(BF16).astype(F32)
            mix[c] = jnp.where(takes_low, coeff - top, top).astype(BF16)

        def second(c):
            local = jnp.dot(back, mix[c], preferred_element_type=F32)
            total = None
            for m in range(members):
                at = slice(m * width, (m + 1) * width)
                term = ens_ref[m, c].astype(F32) * local[:, at]
                total = term if total is None else total + term
            res[:, c] = (total * scale).reshape(groups, here, width)

        def phase_one(i, carry):
            copy(i).wait()
            for j in range(part):
                first(i * part + j)
            return carry

        def phase_two(i, carry):
            for j in range(part):
                second(i * part + j)
            return carry

        lax.fori_loop(0, chunks, phase_one, 0)
        lax.fori_loop(0, chunks, phase_two, 0)
        for k in range(groups):
            block = res[jnp.bitwise_xor(me, k)]
            out = outs[k % 2]
            out[pl.ds(k // 2 * coarse, coarse)] = block.astype(out.dtype)

    shape = (coarse, here, width)
    rows_out = (groups // 2 * coarse, here, width)
    outs = [
        jax.ShapeDtypeStruct(rows_out, F32),
        jax.ShapeDtypeStruct(rows_out, BF16),
    ]
    return call(
        body,
        outs,
        [HB] + [VM] * (1 + groups),
        [
            pltpu.VMEM((members, coarse, levels, width), BF16),
            pltpu.VMEM((groups,) + shape, F32),
            pltpu.VMEM((groups,) + shape, F32),
            pltpu.VMEM((coarse, rows, members * width), BF16),
            pltpu.SemaphoreType.DMA((chunks,)),
        ],
        members * parts[0].size * groups * 64,
        members * parts[0].size * groups * 2,
    )(ensemble, modes, *parts)


def expand(pieces, interp, target):
    owners = len(pieces)
    coarse, levels, width = pieces[0].shape
    fine = interp.shape[0]

    def body(row_ref, int_ref, *refs):
        out_ref, table = refs[-2:]
        me = lax.axis_index("space")
        for k in range(owners):
            at = jnp.bitwise_xor(me, k) * coarse
            table[pl.ds(at, coarse)] = refs[k][...]

        def step(p, carry):
            b = 2 * p
            pair = two_dots(table[row_ref[b]], table[row_ref[b + 1]], int_ref, b)
            out_ref[b], out_ref[b + 1] = pair
            return carry

        lax.fori_loop(0, fine // 2, step, 0, unroll=24)

    return call(
        body,
        jax.ShapeDtypeStruct((fine, levels, width), F32),
        [SM, VM] + [VM] * owners,
        [pltpu.VMEM((owners * coarse, levels, width), BF16)],
        2 * fine * levels * width * width,
        2 * interp.size,
    )(target, interp, *pieces)


def swap(value, axis, size, k):
    return lax.ppermute(value, axis, [(i, i ^ k) for i in range(size)])


def gather_members(value, groups):
    parts, order = [value], [0]
    step = groups // 2
    while step:
        parts = parts + [swap(v, "member", groups, step) for v in parts]
        order = order + [v ^ step for v in order]
        step //= 2
    return [parts[order.index(k)] for k in range(groups)]


def gather_space(value, owners, inner):
    outer = owners // inner

    def send(part, k):
        return swap(part, "space", owners, k)

    pieces = {0: value}
    for i in reversed(range(2, outer)):
        pieces[i * inner] = send(value, i * inner)
    for k in range(1, inner):
        pieces[inner + k] = send(value, inner + k)
    pieces[inner] = send(value, inner)
    for k in range(1, inner):
        pieces[k] = send(value, k)
    for i in reversed(range(2, outer)):
        for k in range(1, inner):
            pieces[i * inner + k] = send(pieces[i * inner], k)
    return [pieces[k] for k in range(owners)]


DIRECT = 0.5
RESTRICT_MIB = 52


def on_device(increment, interp, owner, local_block, ensemble, modes):
    owners = lax.axis_size("space")
    groups = lax.axis_size("member")
    coarse = ensemble.shape[1]
    target = owner.reshape(-1) * coarse + local_block
    inner = 1 << ((owners.bit_length() - 1) // 2)
    outer = owners // inner
    cut = int(coarse * DIRECT)
    plan = [(0, cut, False), (cut, coarse - cut, True)]
    plan = [entry for entry in plan if entry[1]]
    scale = 1.0 / (ensemble.shape[0] * groups - 1)

    sums = restrict(increment, interp, target, plan, coarse, owners, inner)
    flipped = transposed(interp)
    direct, staged = (sums[:owners], sums[owners:]) if cut else ([], sums)

    def send(value, k):
        return swap(value, "space", owners, k)

    sets, near, arrived, second = [], [], {}, {}
    if staged:
        near = [send(v, k + 1) for k, v in enumerate(staged[1:])]
    if direct:
        for k in range(owners // 2, owners):
            arrived[k] = send(direct[k], k)
    if staged:
        mine, *sends = staged_total([(staged[0], near)], outer)
        for i in reversed(range(1, outer)):
            second[i] = send(sends[i - 1], i * inner)
    if direct:
        for k in reversed(range(1, owners // 2)):
            arrived[k] = send(direct[k], k)
        sets.append((direct[0], [arrived[k] for k in range(1, owners)]))
    if staged:
        sets.append((mine, [second[i] for i in range(1, outer)]))
    groups_of = []
    for (start, _, _), entry in zip(plan, sets):
        parts = gather_members(total_of([entry], F32), groups)
        even, odd = covariance(ensemble, modes.T, parts, scale, start)
        groups_of.append((even, [swap(odd, "member", groups, 1)]))
    mine, *sends = staged_total(groups_of, groups // 2)
    arrived = [swap(v, "member", groups, 2 * k + 2) for k, v in enumerate(sends)]
    applied = total_of([(mine, arrived)], BF16)
    pieces = gather_space(applied, owners, inner)
    return expand(pieces, flipped, target)


def solution(mesh):
    in_specs = (
        P("space", "member", None),
        P("space", None, None),
        P("space", None),
        P("space"),
        P("member", "space", None, None),
        P(),
    )
    out_specs = P("space", "member", None)

    return jax.shard_map(
        on_device, mesh=mesh, in_specs=in_specs, out_specs=out_specs, check_vma=False
    )
```
